128 devices in a mesh: row: 8 (over x, core), col: 16 (over z, y).
Axes of the slice: x: 4, y: 4, z: 4, core: 2. Of those that a mesh axis runs over, the one named last changes fastest.
Arguments:
- tail_vectors: float32 [64512, 4096], P('row', 'col'), may hold values from -6 to 6
- lower_panel: float32 [64512, 1024], P(('row', 'col')), may hold values from -0.0234375 to 0.0234375
- window_rhs: float32 [1024, 4096], P('row', 'col'), may hold values from -6 to 6
- window_block: float32 [1024, 1024], P(('row', 'col')), may hold values from -1 to 2, as said below
Outputs:
- window_vectors: float32 [1024, 4096], P('row', 'col')
The draws below stay inside these ranges and needn't reach their ends.
Inputs may be any that keep to these rules, and one draw needn't show every extreme that they name: window_block is zero above the diagonal; its diagonal lies in 1 to 2; entries below the diagonal are under 1 / sqrt(1024) in magnitude.
All inputs are finite; a program needn't handle non-finite values.
Results may differ from the reference program's by a relative error of at most 0.000082.
Values sent between devices are 32-bit elements; how exact they have to be, the bound alone decides.
No kernel may reach another device: no remote copies, remote signals or barrier semaphores. Data moves between devices by JAX's collectives and lax.ppermute only.
A program may use at most 128 MiB of HBM per device.

```python
import jax
import jax.numpy as jnp
from jax import lax

NEV = 4096
WIN = 1024
TAIL = 64512


def draw_window_block(key, part):
    key_lower = jax.random.fold_in(key, 11)
    key_diag = jax.random.fold_in(key, 12)
    lower_mask = jnp.tril(jnp.ones((WIN, WIN), jnp.float32), -1)
    magnitude = 1.0 / jnp.sqrt(jnp.float32(WIN))
    spread = 0.98 * jax.random.uniform(key_lower, (WIN, WIN), jnp.float32, -1.0, 1.0)
    diagonal = jnp.exp(jax.random.uniform(key_diag, (WIN,), jnp.float32, 0.0, 0.69))
    return lower_mask * spread * magnitude + jnp.diag(diagonal)


def shard_levels(key, dims, cuts, smallest, high):
    factor_of, own = 1.0, jax.random.fold_in(key, 6)
    for position, parts in cuts:
        steps = jnp.exp(jax.random.uniform(jax.random.fold_in(own, position), (parts,), jnp.float32, smallest / len(cuts), high / len(cuts)))
        factor_of = factor_of * jnp.repeat(steps, dims[position] // parts).reshape([-1 if axis == position else 1 for axis in range(len(dims))])
    return factor_of


def centred(own_key, extent, scale, limit, shards=(), kind=jnp.bfloat16):
    drawn = jax.random.normal(own_key, extent, jnp.float32) * scale
    if len(shards) > 0:
        drawn = shard_levels(own_key, extent, shards, -0.22, 0.18) * drawn
    return jnp.clip(drawn, min=-limit, max=limit).astype(kind)


def setup_inputs(seed: int = 0) -> dict:
    key_list = jax.random.split(jax.random.key(seed), 5)
    return {
        "tail_vectors": centred(key_list[0], (TAIL, NEV), 1.0, 6.0, ((0, 8), (1, 16)), jnp.float32),
        "lower_panel": centred(key_list[1], (TAIL, WIN), TAIL ** -0.5, 0.0234375, ((0, 128),), jnp.float32),
        "window_rhs": centred(key_list[2], (WIN, NEV), 1.0, 6.0, ((0, 8), (1, 16)), jnp.float32),
        "window_block": draw_window_block(jax.random.fold_in(key_list[4], 71), 0),
    }


def reference(tail_vectors, lower_panel, window_rhs, window_block):
    correction = lax.dot_general(lower_panel.astype(jnp.float32), tail_vectors.astype(jnp.float32), (((0,), (0,)), ((), ())), precision=lax.Precision.HIGHEST, preferred_element_type=jnp.float32)
    right_side = window_rhs - correction
    return jax.scipy.linalg.solve_triangular(window_block, right_side, trans=1, lower=True)
```

```python
import jax
import jax.numpy as jnp
from jax import lax
from jax.sharding import Mesh, PartitionSpec as P

HIGH = lax.Precision.HIGH
HIGHEST = lax.Precision.HIGHEST


def shift(value, axis, by):
    n = lax.axis_size(axis)
    return lax.ppermute(value, axis, [(i, (i + by) % n) for i in range(n)])


def ring_pieces(value, axis):
    return value, shift(value, axis, 1), shift(value, axis, -1), shift(value, axis, 2)


def in_order(pieces, axis):
    own, left, right, far = pieces
    i = lax.axis_index(axis)
    rel = jnp.stack([own, right, far, left] * 2)
    return lax.dynamic_slice_in_dim(rel, (4 - i) % 4, 4, 0)


def dot_t(a, b, precision=HIGH):
    return lax.dot_general(a, b, (((0,), (0,)), ((), ())), precision=precision, preferred_element_type=jnp.float32)


def mm(a, b, precision=HIGHEST):
    return jnp.matmul(a, b, precision=precision, preferred_element_type=jnp.float32)


def invert_blocks(diag):
    nb, s, _ = diag.shape
    rows = lax.broadcasted_iota(jnp.int32, (1, s, s), 1)
    cols = lax.broadcasted_iota(jnp.int32, (1, s, s), 2)
    inv = jnp.where(rows == cols, 1.0 / jnp.where(rows == cols, diag, 1.0), 0.0)
    size = 1
    while size < s:
        low = (rows // (2 * size) == cols // (2 * size)) & (rows // size != cols // size) & (rows > cols)
        inv = inv - mm(mm(inv, jnp.where(low, diag, 0.0)), inv)
        size *= 2
    return inv


def invert_lower(block, base):
    n = block.shape[0]
    nb = n // base
    diag = jnp.stack([block[i * base:(i + 1) * base, i * base:(i + 1) * base] for i in range(nb)])
    level = [m for m in invert_blocks(diag)]
    size = base
    while len(level) > 1:
        merged = []
        for i in range(0, len(level), 2):
            a, d = level[i], level[i + 1]
            low = block[(i + 1) * size:(i + 2) * size, i * size:(i + 1) * size]
            corner = -mm(mm(d, low), a)
            top = jnp.concatenate([a, jnp.zeros_like(a)], axis=1)
            bottom = jnp.concatenate([corner, d], axis=1)
            merged.append(jnp.concatenate([top, bottom], axis=0))
        level = merged
        size *= 2
    return level[0]


def gather_window(block):
    n = block.shape[1]
    part = in_order(ring_pieces(block, "y"), "y").reshape(-1, n)
    part = in_order(ring_pieces(part, "z"), "z").reshape(-1, n)
    part = in_order(ring_pieces(part, "x"), "x")
    other = shift(part, "core", 1)
    core = lax.axis_index("core")
    first = jnp.where(core == 0, part, other)
    second = jnp.where(core == 0, other, part)
    return jnp.stack([first, second], axis=1).reshape(n, n)


def per_device(tail, panel, rhs, block):
    k, n = panel.shape
    cols = tail.shape[1]
    z, y = lax.axis_index("z"), lax.axis_index("y")
    x, core = lax.axis_index("x"), lax.axis_index("core")
    rows = rhs.shape[0]
    tail = tail.reshape(4, 4, k, cols)

    def rows_of(dz):
        by = [lax.dynamic_slice(tail, ((z + dz) % 4, (y + dy) % 4, 0, 0), (1, 1, k, cols)).reshape(k, cols) for dy in (0, -1 % 4, 1, 2)]
        return jnp.concatenate(by, axis=0)

    left, right = shift(panel, "y", 1), shift(panel, "y", -1)
    half = (k // 2) // 8 * 8
    t_left, t_right = shift(rows_of(1), "z", 1), shift(rows_of(3), "z", -1)
    far = jnp.concatenate([shift(left[:half], "y", 1), shift(right[half:], "y", -1)], axis=0)
    t_far = shift(rows_of(2), "z", 2)
    t_own = rows_of(0)
    full = gather_window(block)
    inverse = invert_lower(full, 128)

    near = jnp.concatenate([panel, left, right], axis=0)

    def partial(t):
        return dot_t(near, t[:3 * k]) + dot_t(far, t[3 * k:])

    def reduce_rows(part):
        c = part.shape[1]
        part = part.reshape(4, 2, rows, c)
        mine = lax.dynamic_slice_in_dim(part, core, 1, 1)[:, 0]
        away = lax.dynamic_slice_in_dim(part, 1 - core, 1, 1)[:, 0]
        part = mine + shift(away, "core", 1)
        at = lambda d: lax.dynamic_slice_in_dim(part, (x + d) % 4, 1, 0)[0]
        return at(0) + shift(at(1), "x", 1) + shift(at(3), "x", -1) + shift(at(2), "x", 2)

    def chunk(t, add=None):
        c = -partial(t)
        if add is not None:
            c = lax.dynamic_update_slice_in_dim(c, lax.dynamic_slice_in_dim(c, (x * 2 + core) * rows, rows, 0) + add, (x * 2 + core) * rows, 0)
        return reduce_rows(dot_t(inverse, c))

    own = chunk(t_own, rhs)
    from_right = shift(chunk(t_left), "z", -1)
    from_left = shift(chunk(t_right), "z", 1)
    from_far = shift(chunk(t_far), "z", 2)
    return own + from_right + from_left + from_far


def solution(mesh):
    fine = Mesh(mesh.devices.reshape(4, 2, 4, 4), ("x", "core", "z", "y"))
    row, col = ("x", "core"), ("z", "y")
    in_specs = (P(row, col), P(row + col, None), P(row, col), P(row + col, None))
    return jax.shard_map(per_device, mesh=fine, in_specs=in_specs, out_specs=P(row, col), check_vma=False)
```

```python
import jax
import jax.numpy as jnp
from jax import lax
from jax.experimental import pallas as pl
from jax.experimental.pallas import tpu as pltpu
from jax.sharding import Mesh, PartitionSpec as P


HIGHEST = lax.Precision.HIGHEST
F32, BF16 = jnp.float32, jnp.bfloat16
TILE = 256


def shift(value, axis, by):
    n = lax.axis_size(axis)
    return lax.ppermute(value, axis, [(i, (i + by) % n) for i in range(n)])


def whole(n=1):
    return [pl.BlockSpec(memory_space=pltpu.VMEM)] * n


def scalars_spec():
    return pl.BlockSpec(memory_space=pltpu.SMEM)


def pick(tail, index, sizes):
    _, k, cols = tail.shape
    slots = [(o, j) for o, m in enumerate(sizes) for j in range(m)]

    def body(s_ref, t_ref, *refs):
        outs, buf, sem_in, sem_out = refs[:-3], refs[-3], refs[-2], refs[-1]
        reads = [pltpu.make_async_copy(t_ref.at[s_ref[i]], buf.at[i], sem_in.at[i]) for i in range(len(slots))]
        writes = [pltpu.make_async_copy(buf.at[i], outs[o].at[j], sem_out.at[i]) for i, (o, j) in enumerate(slots)]
        for c in reads:
            c.start()
        for r, w in zip(reads, writes):
            r.wait()
            w.start()
        for w in writes:
            w.wait()

    sems = pltpu.SemaphoreType.DMA((len(slots),))
    return pl.pallas_call(
        body,
        in_specs=[scalars_spec(), pl.BlockSpec(memory_space=pl.ANY)],
        out_specs=[pl.BlockSpec(memory_space=pl.ANY)] * len(sizes),
        out_shape=[jax.ShapeDtypeStruct((m, k, cols), F32) for m in sizes],
        scratch_shapes=[pltpu.VMEM((len(slots), k, cols), F32), sems, sems])(index, tail)


def place(pieces, at):
    r, n = pieces[0].shape

    def body(s_ref, *refs):
        for j, p in enumerate(refs[:-1]):
            refs[-1][pl.ds(pl.multiple_of(s_ref[j] * r, r), r), :] = p[...]

    return pl.pallas_call(
        body, in_specs=[scalars_spec()] + whole(len(pieces)), out_specs=whole()[0],
        out_shape=jax.ShapeDtypeStruct((len(pieces) * r, n), F32))(at, *pieces)


def invert(pieces, at):
    s, n = pieces[0].shape
    nb = n // s

    def exact(a, b):
        return jnp.dot(a, b, precision=HIGHEST, preferred_element_type=F32)

    def body(s_ref, *refs):
        p_refs, o_ref, w_ref = refs[:nb], refs[nb], refs[nb + 1]
        for j in range(nb):
            w_ref[pl.ds(pl.multiple_of(s_ref[j] * s, s), s), :] = p_refs[j][...]
        o_ref[...] = jnp.zeros((n, n), F32)
        rows = lax.broadcasted_iota(jnp.int32, (s, s), 0)
        cols = lax.broadcasted_iota(jnp.int32, (s, s), 1)
        diag = [w_ref[i * s:(i + 1) * s, i * s:(i + 1) * s] for i in range(nb)]
        inv = []
        pair = (rows // 2 == cols // 2) & (rows > cols)
        for d in diag:
            on = jnp.where(rows == cols, d, 0.0)
            by_row = 1.0 / jnp.sum(on, axis=1, keepdims=True)
            by_col = 1.0 / jnp.sum(on, axis=0, keepdims=True)
            inv.append(jnp.where(rows == cols, by_row, 0.0) - jnp.where(pair, d, 0.0) * by_row * by_col)
        size = 2
        while size < s:
            low = (rows // (2 * size) == cols // (2 * size)) & (rows // size != cols // size) & (rows > cols)
            half = [three(v, jnp.where(low, d, 0.0)) for v, d in zip(inv, diag)]
            inv = [v - three(h, v) for v, h in zip(inv, half)]
            size *= 2
        eye = jnp.where(rows == cols, 1.0, 0.0)
        rest = [eye - exact(jnp.where(rows >= cols, d, 0.0), v) for v, d in zip(inv, diag)]
        inv = [v + three(v, e) for v, e in zip(inv, rest)]
        for i in range(nb):
            o_ref[i * s:(i + 1) * s, i * s:(i + 1) * s] = inv[i]
        size = s
        while size < n:
            for i in range(0, n, 2 * size):
                m = i + size
                d = o_ref[m:m + size, m:m + size]
                a = o_ref[i:m, i:m]
                o_ref[m:m + size, i:m] = -three(three(d, w_ref[m:m + size, i:m]), a)
            size *= 2

    return pl.pallas_call(
        body, in_specs=[scalars_spec()] + whole(nb), out_specs=whole()[0],
        out_shape=jax.ShapeDtypeStruct((n, n), F32), scratch_shapes=[pltpu.VMEM((n, n), F32)],
        cost_estimate=pl.CostEstimate(flops=10 ** 10, transcendentals=0, bytes_accessed=8 << 20))(at, *pieces)


def three(a, b):
    ah, al = split(a)
    bh, bl = split(b)
    return dot3(ah, al, bh, bl)


def split(v):
    hi = v.astype(BF16)
    return hi, (v - hi.astype(F32)).astype(BF16)


def padded(v):
    k = v.shape[0]
    return v if k == TILE else jnp.concatenate([v, jnp.zeros((TILE - k, v.shape[1]), v.dtype)], axis=0)


def dot3(ah, al, bh, bl):
    d = lambda a, b: jnp.dot(a, b, preferred_element_type=F32)
    return d(ah, bh) + (d(ah, bl) + d(al, bh))


def products(here, tails, panels, start=None, rhs=None, inverse=None):
    arrays = []

    def ref_of(v):
        for i, u in enumerate(arrays):
            if u is v:
                return i
        arrays.append(v)
        return len(arrays) - 1

    k, cols = tails[0][0][0].shape[1:]
    n = panels[0][0].shape[1]
    nc, ns = len(tails), len(panels)
    m, steps = nc * cols, n // TILE
    t_at = [(c, j, ref_of(v), blk) for c, chunk in enumerate(tails) for j, (v, blk) in enumerate(chunk)]
    p_at = []
    for j, block in enumerate(panels):
        row = 0
        for p in block:
            p_at.append((j, row, p.shape[0], ref_of(p)))
            row += p.shape[0]
    start_at = None if start is None else ref_of(start)
    rhs_at = None if rhs is None else ref_of(rhs)
    inverse_at = None if inverse is None else ref_of(inverse)
    nin = len(arrays)
    nout = 1 if inverse is None else 2
    ncopies = len(t_at) + len(p_at) + (start is not None) + (rhs is not None) + (steps if inverse is not None else 0)

    def body(s_ref, *refs):
        ins, outs, refs = refs[:nin], refs[nin:nin + nout], list(refs[nin + nout:])
        sem_in, sem_out, tb_ref, pb_ref, th_ref, tl_ref, ph_ref, pl_ref, acc_ref = refs[:9]
        refs = refs[9:]
        st_ref = refs.pop(0) if start is not None else None
        rhs_ref = refs.pop(0) if rhs is not None else None
        count = [0]

        def copy_in(src, dst):
            c = pltpu.make_async_copy(src, dst, sem_in.at[count[0]])
            count[0] += 1
            c.start()
            return c

        t_copies, p_copies, x_copies, out_copies = {}, {}, {}, []
        for j in range(ns):
            for c, jj, i, blk in t_at:
                if jj == j:
                    t_copies[c, j] = copy_in(ins[i].at[blk], tb_ref.at[c * ns + j])
            p_copies[j] = [copy_in(ins[i], pb_ref.at[j, row:row + r]) for jj, row, r, i in p_at if jj == j]
        if start is not None:
            s_copy = copy_in(ins[start_at], st_ref)
        if rhs is not None:
            r_copy = copy_in(ins[rhs_at], rhs_ref)
        if inverse is not None:
            xb_ref, ch_ref, cl_ref = refs[:3]
            ob_refs = refs[3:]
            for s in reversed(range(steps)):
                rows = slice(s * TILE, (s + 1) * TILE)
                x_copies[s] = copy_in(ins[inverse_at].at[rows], xb_ref.at[rows])
        for j in range(ns):
            for c in range(nc):
                t_copies[c, j].wait()
            for c in p_copies[j]:
                c.wait()
            b = j % 2
            for h in range(2):
                q = slice(h * TILE, (h + 1) * TILE)
                cut = slice(h * TILE, min((h + 1) * TILE, k))
                for c in range(nc):
                    mine = slice(c * cols, (c + 1) * cols)
                    th_ref[b, mine, q], tl_ref[b, mine, q] = split(padded(tb_ref[c * ns + j, cut, :]).T)
                ph_ref[b, q, :], pl_ref[b, q, :] = split(padded(pb_ref[j, cut, :]))
            for s in range(steps):
                lanes = slice(s * TILE, (s + 1) * TILE)
                d = dot3(th_ref[b], tl_ref[b], ph_ref[b, :, lanes], pl_ref[b, :, lanes])
                acc_ref[:, lanes] = -d if j == 0 else acc_ref[:, lanes] - d
        if start is not None:
            s_copy.wait()
            acc_ref[...] += st_ref[...]
        if rhs is not None:
            r_copy.wait()
            r = rhs_ref.shape[0]
            own = pl.ds(pl.multiple_of((s_ref[1] * 2 + s_ref[0]) * r, r), r)
            acc_ref[:cols, own] += rhs_ref[...].T
        if inverse is None:
            c = pltpu.make_async_copy(acc_ref, outs[0], sem_out.at[0])
            c.start()
            c.wait()
            return
        ch_ref[...], cl_ref[...] = split(acc_ref[...])
        core, x = s_ref[0], s_ref[1]
        swap = core == 1
        half = TILE // 2
        for s in reversed(range(steps)):
            x_copies[s].wait()
            rows = slice(s * TILE, (s + 1) * TILE)
            xh, xl = split(xb_ref[rows, :(s + 1) * TILE])
            for p in range(s + 1):
                lanes = slice(p * TILE, (p + 1) * TILE)
                d = dot3(ch_ref[:, rows], cl_ref[:, rows], xh[:, lanes], xl[:, lanes])
                acc_ref[:, lanes] = d if s == steps - 1 else acc_ref[:, lanes] + d
            at = (s + 4 - x) % 4
            first = acc_ref[:, s * TILE:s * TILE + half].reshape(nc, cols, half)
            second = acc_ref[:, s * TILE + half:(s + 1) * TILE].reshape(nc, cols, half)
            ob_refs[0][s] = jnp.where(swap, second, first)
            ob_refs[1][s] = jnp.where(swap, first, second)
            for o in range(2):
                c = pltpu.make_async_copy(ob_refs[o].at[s], outs[o].at[at], sem_out.at[2 * s + o])
                c.start()
                out_copies.append(c)
        for c in out_copies:
            c.wait()

    depth = 2 * TILE
    scratch = [
        pltpu.SemaphoreType.DMA((ncopies,)), pltpu.SemaphoreType.DMA((2 * steps,)),
        pltpu.VMEM((nc * ns, k, cols), F32), pltpu.VMEM((ns, k, n), F32),
        pltpu.VMEM((2, m, depth), BF16), pltpu.VMEM((2, m, depth), BF16),
        pltpu.VMEM((2, depth, n), BF16), pltpu.VMEM((2, depth, n), BF16), pltpu.VMEM((m, n), F32)]
    if start is not None:
        scratch.append(pltpu.VMEM((m, n), F32))
    if rhs is not None:
        scratch.append(pltpu.VMEM(rhs.shape, F32))
    flops = 2 * m * depth * ns * n * 3
    if inverse is not None:
        scratch += [pltpu.VMEM((n, n), F32), pltpu.VMEM((m, n), BF16), pltpu.VMEM((m, n), BF16)]
        scratch += [pltpu.VMEM((4, nc, cols, TILE // 2), F32)] * 2
        out_shape = [jax.ShapeDtypeStruct((4, nc, cols, TILE // 2), F32)] * 2
        flops += 2 * m * n * n * 2
    else:
        out_shape = [jax.ShapeDtypeStruct((m, n), F32)]
    anywhere = pl.BlockSpec(memory_space=pl.ANY)
    out = pl.pallas_call(
        body, in_specs=[scalars_spec()] + [anywhere] * nin, out_specs=[anywhere] * nout, out_shape=out_shape,
        scratch_shapes=scratch,
        cost_estimate=pl.CostEstimate(flops=flops, transcendentals=0, bytes_accessed=14 << 20))(here, *arrays)
    return out if inverse is not None else out[0]


def device(tail, panel, rhs, block):
    k, _ = panel.shape
    cols = tail.shape[1]
    z, y = lax.axis_index("z"), lax.axis_index("y")
    x, core = lax.axis_index("x"), lax.axis_index("core")
    tail = tail.reshape(16, k, cols)
    i32 = lambda *v: jnp.stack([jnp.asarray(u, jnp.int32) for u in v])
    order = i32(y, (y + 3) % 4, (y + 1) % 4, (y + 2) % 4)
    here = i32(core, x)
    index = lambda dz: ((z + dz) % 4) * 4 + order
    ring = lambda i: i32(i, (i + 3) % 4, (i + 1) % 4, (i + 2) % 4)

    t0, = pick(tail, index(2)[:1], (1,))
    tf0 = shift(t0, "z", 2)
    wy = place([block, shift(block, "y", 1), shift(block, "y", -1), shift(block, "y", 2)], ring(y))
    top, bottom = panel[:TILE], panel[TILE:]
    l_t, r_b = shift(top, "y", 1), shift(bottom, "y", -1)
    l_b, r_t = shift(bottom, "y", 1), shift(top, "y", -1)
    wz = place([wy, shift(wy, "z", 1), shift(wy, "z", -1), shift(wy, "z", 2)], ring(z))
    tl, tr = pick(tail, jnp.concatenate([index(1), index(3)]), (4, 4))
    t1, t2, t_own = pick(tail, jnp.concatenate([index(2)[1:], index(0)]), (2, 1, 4))
    t_l = shift(tl, "z", 1)
    t_r = shift(tr, "z", -1)
    tf1 = shift(t1, "z", 2)
    tf2 = shift(t2, "z", 2)
    wx = [wz, shift(wz, "x", 1), shift(wz, "x", -1), shift(wz, "x", 2)]
    wx += [shift(w, "core", 1) for w in wx]
    f_l = shift(l_t, "y", 1)
    f_r = shift(r_b, "y", -1)
    inverse = invert(wx, jnp.concatenate([ring(x) * 2 + core, ring(x) * 2 + 1 - core]))

    near = [[panel], [l_t, l_b], [r_t, r_b]]
    far = [[f_l, f_r]]
    group = [t_own, t_l, t_r]
    c_g = products(here, [[(t, j) for j in range(3)] for t in group], near, rhs=rhs)
    p_g = products(here, [[(t, 3)] for t in group], far, start=c_g, inverse=inverse)
    c_f = products(here, [[(tf0, 0), (tf1, 0), (tf1, 1)]], near)
    p_f = products(here, [[(tf2, 0)]], far, start=c_f, inverse=inverse)

    def over_rows(parts):
        mine, away = parts
        s = mine + shift(away, "core", 1)
        return (s[0] + shift(s[1], "x", 1)) + (shift(s[3], "x", -1) + shift(s[2], "x", 2))

    g = over_rows(p_g)
    h = over_rows(p_f)
    out = (g[0] + shift(g[1], "z", -1)) + (shift(g[2], "z", 1) + shift(h[0], "z", 2))
    return out.T


def solution(mesh):
    fine = Mesh(mesh.devices.reshape(4, 2, 4, 4), ("x", "core", "z", "y"))
    row, col = ("x", "core"), ("z", "y")
    in_specs = (P(row, col), P(row + col, None), P(row, col), P(row + col, None))
    return jax.shard_map(device, mesh=fine, in_specs=in_specs, out_specs=P(row, col), check_vma=False)
```

```python
import jax
import jax.numpy as jnp
from jax import lax
from jax.experimental import pallas as pl
from jax.experimental.pallas import tpu as pltpu
from jax.sharding import Mesh, PartitionSpec as P


HIGHEST = lax.Precision.HIGHEST
F32, BF16 = jnp.float32, jnp.bfloat16
TILE = 256


def shift(value, axis, by):
    n = lax.axis_size(axis)
    return lax.ppermute(value, axis, [(i, (i + by) % n) for i in range(n)])


def whole(n=1):
    return [pl.BlockSpec(memory_space=pltpu.VMEM)] * n


def scalars_spec():
    return pl.BlockSpec(memory_space=pltpu.SMEM)


def pick(tail, index, sizes):
    _, k, cols = tail.shape
    slots = [(o, j) for o, m in enumerate(sizes) for j in range(m)]

    def body(s_ref, t_ref, *refs):
        outs, buf, sem_in, sem_out = refs[:-3], refs[-3], refs[-2], refs[-1]
        reads = [pltpu.make_async_copy(t_ref.at[s_ref[i]], buf.at[i], sem_in.at[i]) for i in range(len(slots))]
        writes = [pltpu.make_async_copy(buf.at[i], outs[o].at[j], sem_out.at[i]) for i, (o, j) in enumerate(slots)]
        for c in reads:
            c.start()
        for r, w in zip(reads, writes):
            r.wait()
            w.start()
        for w in writes:
            w.wait()

    sems = pltpu.SemaphoreType.DMA((len(slots),))
    return pl.pallas_call(
        body,
        in_specs=[scalars_spec(), pl.BlockSpec(memory_space=pl.ANY)],
        out_specs=[pl.BlockSpec(memory_space=pl.ANY)] * len(sizes),
        out_shape=[jax.ShapeDtypeStruct((m, k, cols), F32) for m in sizes],
        scratch_shapes=[pltpu.VMEM((len(slots), k, cols), F32), sems, sems])(index, tail)


def place(pieces, at):
    r, n = pieces[0].shape

    def body(s_ref, *refs):
        for j, p in enumerate(refs[:-1]):
            refs[-1][pl.ds(pl.multiple_of(s_ref[j] * r, r), r), :] = p[...]

    return pl.pallas_call(
        body, in_specs=[scalars_spec()] + whole(len(pieces)), out_specs=whole()[0],
        out_shape=jax.ShapeDtypeStruct((len(pieces) * r, n), F32))(at, *pieces)


def invert(pieces, at):
    s, n = pieces[0].shape
    nb = n // s

    def exact(a, b):
        return jnp.dot(a, b, precision=HIGHEST, preferred_element_type=F32)

    def body(s_ref, *refs):
        p_refs, o_ref, w_ref = refs[:nb], refs[nb], refs[nb + 1]
        for j in range(nb):
            w_ref[pl.ds(pl.multiple_of(s_ref[j] * s, s), s), :] = p_refs[j][...]
        o_ref[...] = jnp.zeros((n, n), F32)
        rows = lax.broadcasted_iota(jnp.int32, (s, s), 0)
        cols = lax.broadcasted_iota(jnp.int32, (s, s), 1)
        diag = [w_ref[i * s:(i + 1) * s, i * s:(i + 1) * s] for i in range(nb)]
        inv = []
        pair = (rows // 2 == cols // 2) & (rows > cols)
        for d in diag:
            on = jnp.where(rows == cols, d, 0.0)
            by_row = 1.0 / jnp.sum(on, axis=1, keepdims=True)
            by_col = 1.0 / jnp.sum(on, axis=0, keepdims=True)
            inv.append(jnp.where(rows == cols, by_row, 0.0) - jnp.where(pair, d, 0.0) * by_row * by_col)
        size = 2
        while size < s:
            low = (rows // (2 * size) == cols // (2 * size)) & (rows // size != cols // size) & (rows > cols)
            half = [three(v, jnp.where(low, d, 0.0)) for v, d in zip(inv, diag)]
            inv = [v - three(h, v) for v, h in zip(inv, half)]
            size *= 2
        eye = jnp.where(rows == cols, 1.0, 0.0)
        rest = [eye - exact(jnp.where(rows >= cols, d, 0.0), v) for v, d in zip(inv, diag)]
        inv = [v + three(v, e) for v, e in zip(inv, rest)]
        for i in range(nb):
            o_ref[i * s:(i + 1) * s, i * s:(i + 1) * s] = inv[i]
        size = s
        while size < n:
            for i in range(0, n, 2 * size):
                m = i + size
                d = o_ref[m:m + size, m:m + size]
                a = o_ref[i:m, i:m]
                o_ref[m:m + size, i:m] = -three(three(d, w_ref[m:m + size, i:m]), a)
            size *= 2

    return pl.pallas_call(
        body, in_specs=[scalars_spec()] + whole(nb), out_specs=whole()[0],
        out_shape=jax.ShapeDtypeStruct((n, n), F32), scratch_shapes=[pltpu.VMEM((n, n), F32)],
        cost_estimate=pl.CostEstimate(flops=10 ** 10, transcendentals=0, bytes_accessed=8 << 20))(at, *pieces)


def three(a, b):
    ah, al = split(a)
    bh, bl = split(b)
    return dot3(ah, al, bh, bl)


def split(v):
    hi = v.astype(BF16)
    return hi, (v - hi.astype(F32)).astype(BF16)


def padded(v):
    k = v.shape[0]
    return v if k == TILE else jnp.concatenate([v, jnp.zeros((TILE - k, v.shape[1]), v.dtype)], axis=0)


def dot3(ah, al, bh, bl):
    d = lambda a, b: jnp.dot(a, b, preferred_element_type=F32)
    return d(ah, bh) + (d(ah, bl) + d(al, bh))


def products(here, tails, panels, start=None, rhs=None, inverse=None):
    arrays = []

    def ref_of(v):
        for i, u in enumerate(arrays):
            if u is v:
                return i
        arrays.append(v)
        return len(arrays) - 1

    k, cols = tails[-1][0][0].shape[1:]
    n = panels[0][0].shape[1]
    nc, ns = len(tails), len(panels)
    m, steps = nc * cols, n // TILE
    t_at = [(c, j, ref_of(t[0]), t[1]) for c, chunk in enumerate(tails) for j, t in enumerate(chunk) if t is not None]
    skip = [sum(chunk[j] is None for chunk in tails) for j in range(ns)]
    p_at = []
    for j, block in enumerate(panels):
        row = 0
        for p in block:
            p_at.append((j, row, p.shape[0], ref_of(p)))
            row += p.shape[0]
    start, start_row, start_rows = (None, 0, 0) if start is None else start
    start_at = None if start is None else ref_of(start)
    rhs_at = None if rhs is None else ref_of(rhs)
    inverse_at = None if inverse is None else ref_of(inverse)
    nin = len(arrays)
    nout = 1 if inverse is None else 2
    ncopies = len(t_at) + len(p_at) + (start is not None) + (rhs is not None) + (steps if inverse is not None else 0)

    def body(s_ref, *refs):
        ins, outs, refs = refs[:nin], refs[nin:nin + nout], list(refs[nin + nout:])
        sem_in, sem_out, tb_ref, pb_ref, th_ref, tl_ref, ph_ref, pl_ref, acc_ref = refs[:9]
        refs = refs[9:]
        st_ref = refs.pop(0) if start is not None else None
        rhs_ref = refs.pop(0) if rhs is not None else None
        count = [0]

        def copy_in(src, dst):
            c = pltpu.make_async_copy(src, dst, sem_in.at[count[0]])
            count[0] += 1
            c.start()
            return c

        t_copies, p_copies, x_copies, out_copies = {}, {}, {}, []
        for j in range(ns):
            for c, jj, i, blk in t_at:
                if jj == j:
                    t_copies[c, j] = copy_in(ins[i].at[blk], tb_ref.at[c * ns + j])
            p_copies[j] = [copy_in(ins[i], pb_ref.at[j, row:row + r]) for jj, row, r, i in p_at if jj == j]
        if start is not None:
            s_copy = copy_in(ins[start_at].at[start_row:start_row + start_rows], st_ref)
        if rhs is not None:
            r_copy = copy_in(ins[rhs_at], rhs_ref)
        if inverse is not None:
            xb_ref, ch_ref, cl_ref = refs[:3]
            ob_refs = refs[3:]
            for s in reversed(range(steps)):
                rows = slice(s * TILE, (s + 1) * TILE)
                x_copies[s] = copy_in(ins[inverse_at].at[rows], xb_ref.at[rows])
        for j in range(ns):
            low = skip[j] * cols
            for c in range(skip[j], nc):
                t_copies[c, j].wait()
            for c in p_copies[j]:
                c.wait()
            b = j % 2
            for h in range(2):
                q = slice(h * TILE, (h + 1) * TILE)
                cut = slice(h * TILE, min((h + 1) * TILE, k))
                for c in range(skip[j], nc):
                    mine = slice(c * cols, (c + 1) * cols)
                    th_ref[b, mine, q], tl_ref[b, mine, q] = split(padded(tb_ref[c * ns + j, cut, :]).T)
                ph_ref[b, q, :], pl_ref[b, q, :] = split(padded(pb_ref[j, cut, :]))
            for s in range(steps):
                lanes = slice(s * TILE, (s + 1) * TILE)
                d = dot3(th_ref[b, low:], tl_ref[b, low:], ph_ref[b, :, lanes], pl_ref[b, :, lanes])
                acc_ref[low:, lanes] = -d if j == 0 else acc_ref[low:, lanes] - d
                if j == 0 and low:
                    acc_ref[:low, lanes] = jnp.zeros((low, TILE), F32)
        if start is not None:
            s_copy.wait()
            acc_ref[:start_rows, :] += st_ref[...]
        if rhs is not None:
            r_copy.wait()
            r = rhs_ref.shape[0]
            own = pl.ds(pl.multiple_of((s_ref[1] * 2 + s_ref[0]) * r, r), r)
            acc_ref[:cols, own] += rhs_ref[...].T
        if inverse is None:
            c = pltpu.make_async_copy(acc_ref, outs[0], sem_out.at[0])
            c.start()
            c.wait()
            return
        ch_ref[...], cl_ref[...] = split(acc_ref[...])
        core, x = s_ref[0], s_ref[1]
        swap = core == 1
        half = TILE // 2
        for s in reversed(range(steps)):
            x_copies[s].wait()
            rows = slice(s * TILE, (s + 1) * TILE)
            xh, xl = split(xb_ref[rows, :(s + 1) * TILE])
            for p in range(s + 1):
                lanes = slice(p * TILE, (p + 1) * TILE)
                d = dot3(ch_ref[:, rows], cl_ref[:, rows], xh[:, lanes], xl[:, lanes])
                acc_ref[:, lanes] = d if s == steps - 1 else acc_ref[:, lanes] + d
            at = (s + 4 - x) % 4
            first = acc_ref[:, s * TILE:s * TILE + half].reshape(nc, cols, half)
            second = acc_ref[:, s * TILE + half:(s + 1) * TILE].reshape(nc, cols, half)
            ob_refs[0][s] = jnp.where(swap, second, first)
            ob_refs[1][s] = jnp.where(swap, first, second)
            for o in range(2):
                c = pltpu.make_async_copy(ob_refs[o].at[s], outs[o].at[at], sem_out.at[2 * s + o])
                c.start()
                out_copies.append(c)
        for c in out_copies:
            c.wait()

    depth = 2 * TILE
    scratch = [
        pltpu.SemaphoreType.DMA((ncopies,)), pltpu.SemaphoreType.DMA((2 * steps,)),
        pltpu.VMEM((nc * ns, k, cols), F32), pltpu.VMEM((ns, k, n), F32),
        pltpu.VMEM((2, m, depth), BF16), pltpu.VMEM((2, m, depth), BF16),
        pltpu.VMEM((2, depth, n), BF16), pltpu.VMEM((2, depth, n), BF16), pltpu.VMEM((m, n), F32)]
    if start is not None:
        scratch.append(pltpu.VMEM((start_rows, n), F32))
    if rhs is not None:
        scratch.append(pltpu.VMEM(rhs.shape, F32))
    flops = 2 * m * depth * ns * n * 3
    if inverse is not None:
        scratch += [pltpu.VMEM((n, n), F32), pltpu.VMEM((m, n), BF16), pltpu.VMEM((m, n), BF16)]
        scratch += [pltpu.VMEM((4, nc, cols, TILE // 2), F32)] * 2
        out_shape = [jax.ShapeDtypeStruct((4, nc, cols, TILE // 2), F32)] * 2
        flops += 2 * m * n * n * 2
    else:
        out_shape = [jax.ShapeDtypeStruct((m, n), F32)]
    anywhere = pl.BlockSpec(memory_space=pl.ANY)
    out = pl.pallas_call(
        body, in_specs=[scalars_spec()] + [anywhere] * nin, out_specs=[anywhere] * nout, out_shape=out_shape,
        scratch_shapes=scratch,
        cost_estimate=pl.CostEstimate(flops=flops, transcendentals=0, bytes_accessed=14 << 20))(here, *arrays)
    return out if inverse is not None else out[0]


def device(tail, panel, rhs, block):
    k, _ = panel.shape
    cols = tail.shape[1]
    z, y = lax.axis_index("z"), lax.axis_index("y")
    x, core = lax.axis_index("x"), lax.axis_index("core")
    tail = tail.reshape(16, k, cols)
    i32 = lambda *v: jnp.stack([jnp.asarray(u, jnp.int32) for u in v])
    order = i32(y, (y + 3) % 4, (y + 1) % 4, (y + 2) % 4)
    here = i32(core, x)
    index = lambda dz: ((z + dz) % 4) * 4 + order
    ring = lambda i: i32(i, (i + 3) % 4, (i + 1) % 4, (i + 2) % 4)

    t0, = pick(tail, index(2)[:1], (1,))
    tf0 = shift(t0, "z", 2)
    wy = place([block, shift(block, "y", 1), shift(block, "y", -1), shift(block, "y", 2)], ring(y))
    top, bottom = panel[:TILE], panel[TILE:]
    l_t, r_b = shift(top, "y", 1), shift(bottom, "y", -1)
    l_b, r_t = shift(bottom, "y", 1), shift(top, "y", -1)
    wz = place([wy, shift(wy, "z", 1), shift(wy, "z", -1), shift(wy, "z", 2)], ring(z))
    tl, tr = pick(tail, jnp.concatenate([index(1), index(3)]), (4, 4))
    t1, t2, t_own = pick(tail, jnp.concatenate([index(2)[1:], index(0)]), (2, 1, 4))
    t_l = shift(tl, "z", 1)
    t_r = shift(tr, "z", -1)
    tf1 = shift(t1, "z", 2)
    tf2 = shift(t2, "z", 2)
    wx = [wz, shift(wz, "x", 1), shift(wz, "x", -1), shift(wz, "x", 2)]
    wx += [shift(w, "core", 1) for w in wx]
    f_l = shift(l_t, "y", 1)
    f_r = shift(r_b, "y", -1)
    inverse = invert(wx, jnp.concatenate([ring(x) * 2 + core, ring(x) * 2 + 1 - core]))

    near = [[panel], [l_t, l_b], [r_t, r_b]]
    far = [[f_l, f_r]]
    group = [t_own, t_l, t_r]
    c_0 = products(here, [[(tf0, 0)], [(t_own, 0)]], near[:1])
    c_g = products(
        here, [[None if t is t_own and j == 0 else (t, j) for j in range(3)] for t in group], near,
        start=(c_0, cols, cols), rhs=rhs)
    p_g = products(here, [[(t, 3)] for t in group], far, start=(c_g, 0, 3 * cols), inverse=inverse)
    c_f = products(here, [[(tf1, 0), (tf1, 1)]], near[1:], start=(c_0, 0, cols))
    p_f = products(here, [[(tf2, 0)]], far, start=(c_f, 0, cols), inverse=inverse)

    def over_rows(parts):
        mine, away = parts
        s = mine + shift(away, "core", 1)
        return (s[0] + shift(s[1], "x", 1)) + (shift(s[3], "x", -1) + shift(s[2], "x", 2))

    g = over_rows(p_g)
    h = over_rows(p_f)
    out = (g[0] + shift(g[1], "z", -1)) + (shift(g[2], "z", 1) + shift(h[0], "z", 2))
    return out.T


def solution(mesh):
    fine = Mesh(mesh.devices.reshape(4, 2, 4, 4), ("x", "core", "z", "y"))
    row, col = ("x", "core"), ("z", "y")
    in_specs = (P(row, col), P(row + col, None), P(row, col), P(row + col, None))
    return jax.shard_map(device, mesh=fine, in_specs=in_specs, out_specs=P(row, col), check_vma=False)
```

```python
import jax
import jax.numpy as jnp
from jax import lax
from jax.experimental import pallas as pl
from jax.experimental.pallas import tpu as pltpu
from jax.sharding import Mesh, PartitionSpec as P


HIGHEST = lax.Precision.HIGHEST
F32, BF16 = jnp.float32, jnp.bfloat16
TILE = 256


def shift(value, axis, by):
    n = lax.axis_size(axis)
    return lax.ppermute(value, axis, [(i, (i + by) % n) for i in range(n)])


def whole(n=1):
    return [pl.BlockSpec(memory_space=pltpu.VMEM)] * n


def scalars_spec():
    return pl.BlockSpec(memory_space=pltpu.SMEM)


def pick(tail, index, sizes):
    _, k, cols = tail.shape
    slots = [(o, j) for o, m in enumerate(sizes) for j in range(m)]

    def body(s_ref, t_ref, *refs):
        outs, buf, sem_in, sem_out = refs[:-3], refs[-3], refs[-2], refs[-1]
        reads = [pltpu.make_async_copy(t_ref.at[s_ref[i]], buf.at[i], sem_in.at[i]) for i in range(len(slots))]
        writes = [pltpu.make_async_copy(buf.at[i], outs[o].at[j], sem_out.at[i]) for i, (o, j) in enumerate(slots)]
        for c in reads:
            c.start()
        for r, w in zip(reads, writes):
            r.wait()
            w.start()
        for w in writes:
            w.wait()

    sems = pltpu.SemaphoreType.DMA((len(slots),))
    return pl.pallas_call(
        body,
        in_specs=[scalars_spec(), pl.BlockSpec(memory_space=pl.ANY)],
        out_specs=[pl.BlockSpec(memory_space=pl.ANY)] * len(sizes),
        out_shape=[jax.ShapeDtypeStruct((m, k, cols), F32) for m in sizes],
        scratch_shapes=[pltpu.VMEM((len(slots), k, cols), F32), sems, sems])(index, tail)


def place(pieces, at):
    r, n = pieces[0].shape

    def body(s_ref, *refs):
        for j, p in enumerate(refs[:-1]):
            refs[-1][pl.ds(pl.multiple_of(s_ref[j] * r, r), r), :] = p[...]

    return pl.pallas_call(
        body, in_specs=[scalars_spec()] + whole(len(pieces)), out_specs=whole()[0],
        out_shape=jax.ShapeDtypeStruct((len(pieces) * r, n), F32))(at, *pieces)


def invert(pieces, at):
    s, n = pieces[0].shape
    nb = n // s

    def exact(a, b):
        return jnp.dot(a, b, precision=HIGHEST, preferred_element_type=F32)

    def body(s_ref, *refs):
        p_refs, o_ref, w_ref, i_ref = refs[:nb], refs[nb], refs[nb + 1], refs[nb + 2]
        for j in range(nb):
            w_ref[pl.ds(pl.multiple_of(s_ref[j] * s, s), s), :] = p_refs[j][...]
        o_ref[...] = jnp.zeros((n, n), F32)
        rows = lax.broadcasted_iota(jnp.int32, (s, s), 0)
        cols = lax.broadcasted_iota(jnp.int32, (s, s), 1)
        diag = [w_ref[i * s:(i + 1) * s, i * s:(i + 1) * s] for i in range(nb)]
        pair = (rows // 2 == cols // 2) & (rows > cols)
        for i, d in enumerate(diag):
            on = jnp.where(rows == cols, d, 0.0)
            by_row = 1.0 / jnp.sum(on, axis=1, keepdims=True)
            by_col = 1.0 / jnp.sum(on, axis=0, keepdims=True)
            i_ref[i] = jnp.where(rows == cols, by_row, 0.0) - jnp.where(pair, d, 0.0) * by_row * by_col

        def double(t, _):
            low = ((rows >> (t + 1)) == (cols >> (t + 1))) & ((rows >> t) != (cols >> t)) & (rows > cols)
            half = [three(i_ref[i], jnp.where(low, w_ref[i * s:(i + 1) * s, i * s:(i + 1) * s], 0.0)) for i in range(nb)]
            for i in range(nb):
                i_ref[i] = i_ref[i] - three(half[i], i_ref[i])
            return 0

        lax.fori_loop(1, 5, double, 0)
        inv = [i_ref[i] for i in range(nb)]
        size = 32
        while size < s:
            low = (rows // (2 * size) == cols // (2 * size)) & (rows // size != cols // size) & (rows > cols)
            half = [three(v, jnp.where(low, d, 0.0)) for v, d in zip(inv, diag)]
            inv = [v - three(h, v) for v, h in zip(inv, half)]
            size *= 2
        eye = jnp.where(rows == cols, 1.0, 0.0)
        rest = [eye - exact(jnp.where(rows >= cols, d, 0.0), v) for v, d in zip(inv, diag)]
        inv = [v + three(v, e) for v, e in zip(inv, rest)]
        for i in range(nb):
            o_ref[i * s:(i + 1) * s, i * s:(i + 1) * s] = inv[i]
        size = s
        while size < n:
            for i in range(0, n, 2 * size):
                m = i + size
                d = o_ref[m:m + size, m:m + size]
                a = o_ref[i:m, i:m]
                o_ref[m:m + size, i:m] = -three(three(d, w_ref[m:m + size, i:m]), a)
            size *= 2

    return pl.pallas_call(
        body, in_specs=[scalars_spec()] + whole(nb), out_specs=whole()[0],
        out_shape=jax.ShapeDtypeStruct((n, n), F32), scratch_shapes=[pltpu.VMEM((n, n), F32), pltpu.VMEM((nb, s, s), F32)],
        cost_estimate=pl.CostEstimate(flops=10 ** 10, transcendentals=0, bytes_accessed=8 << 20))(at, *pieces)


def three(a, b):
    ah, al = split(a)
    bh, bl = split(b)
    return dot3(ah, al, bh, bl)


def split(v):
    hi = v.astype(BF16)
    return hi, (v - hi.astype(F32)).astype(BF16)


def padded(v):
    k = v.shape[0]
    return v if k == TILE else jnp.concatenate([v, jnp.zeros((TILE - k, v.shape[1]), v.dtype)], axis=0)


def dot3(ah, al, bh, bl):
    d = lambda a, b: jnp.dot(a, b, preferred_element_type=F32)
    return d(ah, bh) + (d(ah, bl) + d(al, bh))


def products(here, tails, panels, start=None, rhs=None, inverse=None):
    arrays = []

    def ref_of(v):
        for i, u in enumerate(arrays):
            if u is v:
                return i
        arrays.append(v)
        return len(arrays) - 1

    k, cols = tails[-1][0][0].shape[1:]
    n = panels[0][0].shape[1]
    nc, ns = len(tails), len(panels)
    m, steps = nc * cols, n // TILE
    t_at = [(c, j, ref_of(t[0]), t[1]) for c, chunk in enumerate(tails) for j, t in enumerate(chunk) if t is not None]
    skip = [sum(chunk[j] is None for chunk in tails) for j in range(ns)]
    p_at = []
    for j, block in enumerate(panels):
        row = 0
        for p in block:
            p_at.append((j, row, p.shape[0], ref_of(p)))
            row += p.shape[0]
    start, start_row, start_rows = (None, 0, 0) if start is None else start
    start_at = None if start is None else ref_of(start)
    rhs_at = None if rhs is None else ref_of(rhs)
    inverse_at = None if inverse is None else ref_of(inverse)
    nin = len(arrays)
    nout = 1 if inverse is None else 2
    ncopies = len(t_at) + len(p_at) + (start is not None) + (rhs is not None) + (steps if inverse is not None else 0)

    def body(s_ref, *refs):
        ins, outs, refs = refs[:nin], refs[nin:nin + nout], list(refs[nin + nout:])
        sem_in, sem_out, tb_ref, pb_ref, th_ref, tl_ref, ph_ref, pl_ref, acc_ref = refs[:9]
        refs = refs[9:]
        st_ref = refs.pop(0) if start is not None else None
        rhs_ref = refs.pop(0) if rhs is not None else None
        count = [0]

        def copy_in(src, dst):
            c = pltpu.make_async_copy(src, dst, sem_in.at[count[0]])
            count[0] += 1
            c.start()
            return c

        t_copies, p_copies, x_copies, out_copies = {}, {}, {}, []
        for j in range(ns):
            for c, jj, i, blk in t_at:
                if jj == j:
                    t_copies[c, j] = copy_in(ins[i].at[blk], tb_ref.at[c * ns + j])
            p_copies[j] = [copy_in(ins[i], pb_ref.at[j, row:row + r]) for jj, row, r, i in p_at if jj == j]
        if start is not None:
            s_copy = copy_in(ins[start_at].at[start_row:start_row + start_rows], st_ref)
        if rhs is not None:
            r_copy = copy_in(ins[rhs_at], rhs_ref)
        if inverse is not None:
            xb_ref, ch_ref, cl_ref = refs[:3]
            ob_refs = refs[3:]
            for s in reversed(range(steps)):
                rows = slice(s * TILE, (s + 1) * TILE)
                x_copies[s] = copy_in(ins[inverse_at].at[rows], xb_ref.at[rows])
        for j in range(ns):
            low = skip[j] * cols
            for c in range(skip[j], nc):
                t_copies[c, j].wait()
            for c in p_copies[j]:
                c.wait()
            b = j % 2
            for h in range(2):
                q = slice(h * TILE, (h + 1) * TILE)
                cut = slice(h * TILE, min((h + 1) * TILE, k))
                for c in range(skip[j], nc):
                    mine = slice(c * cols, (c + 1) * cols)
                    th_ref[b, mine, q], tl_ref[b, mine, q] = split(padded(tb_ref[c * ns + j, cut, :]).T)
                ph_ref[b, q, :], pl_ref[b, q, :] = split(padded(pb_ref[j, cut, :]))
            for s in range(steps):
                lanes = slice(s * TILE, (s + 1) * TILE)
                d = dot3(th_ref[b, low:], tl_ref[b, low:], ph_ref[b, :, lanes], pl_ref[b, :, lanes])
                acc_ref[low:, lanes] = -d if j == 0 else acc_ref[low:, lanes] - d
                if j == 0 and low:
                    acc_ref[:low, lanes] = jnp.zeros((low, TILE), F32)
        if start is not None:
            s_copy.wait()
            acc_ref[:start_rows, :] += st_ref[...]
        if rhs is not None:
            r_copy.wait()
            r = rhs_ref.shape[0]
            own = pl.ds(pl.multiple_of((s_ref[1] * 2 + s_ref[0]) * r, r), r)
            acc_ref[:cols, own] += rhs_ref[...].T
        if inverse is None:
            c = pltpu.make_async_copy(acc_ref, outs[0], sem_out.at[0])
            c.start()
            c.wait()
            return
        ch_ref[...], cl_ref[...] = split(acc_ref[...])
        core, x = s_ref[0], s_ref[1]
        swap = core == 1
        half = TILE // 2
        for s in reversed(range(steps)):
            x_copies[s].wait()
            rows = slice(s * TILE, (s + 1) * TILE)
            xh, xl = split(xb_ref[rows, :(s + 1) * TILE])
            for p in range(s + 1):
                lanes = slice(p * TILE, (p + 1) * TILE)
                d = dot3(ch_ref[:, rows], cl_ref[:, rows], xh[:, lanes], xl[:, lanes])
                acc_ref[:, lanes] = d if s == steps - 1 else acc_ref[:, lanes] + d
            at = (s + 4 - x) % 4
            first = acc_ref[:, s * TILE:s * TILE + half].reshape(nc, cols, half)
            second = acc_ref[:, s * TILE + half:(s + 1) * TILE].reshape(nc, cols, half)
            ob_refs[0][s] = jnp.where(swap, second, first)
            ob_refs[1][s] = jnp.where(swap, first, second)
            for o in range(2):
                c = pltpu.make_async_copy(ob_refs[o].at[s], outs[o].at[at], sem_out.at[2 * s + o])
                c.start()
                out_copies.append(c)
        for c in out_copies:
            c.wait()

    depth = 2 * TILE
    scratch = [
        pltpu.SemaphoreType.DMA((ncopies,)), pltpu.SemaphoreType.DMA((2 * steps,)),
        pltpu.VMEM((nc * ns, k, cols), F32), pltpu.VMEM((ns, k, n), F32),
        pltpu.VMEM((2, m, depth), BF16), pltpu.VMEM((2, m, depth), BF16),
        pltpu.VMEM((2, depth, n), BF16), pltpu.VMEM((2, depth, n), BF16), pltpu.VMEM((m, n), F32)]
    if start is not None:
        scratch.append(pltpu.VMEM((start_rows, n), F32))
    if rhs is not None:
        scratch.append(pltpu.VMEM(rhs.shape, F32))
    flops = 2 * m * depth * ns * n * 3
    if inverse is not None:
        scratch += [pltpu.VMEM((n, n), F32), pltpu.VMEM((m, n), BF16), pltpu.VMEM((m, n), BF16)]
        scratch += [pltpu.VMEM((4, nc, cols, TILE // 2), F32)] * 2
        out_shape = [jax.ShapeDtypeStruct((4, nc, cols, TILE // 2), F32)] * 2
        flops += 2 * m * n * n * 2
    else:
        out_shape = [jax.ShapeDtypeStruct((m, n), F32)]
    anywhere = pl.BlockSpec(memory_space=pl.ANY)
    out = pl.pallas_call(
        body, in_specs=[scalars_spec()] + [anywhere] * nin, out_specs=[anywhere] * nout, out_shape=out_shape,
        scratch_shapes=scratch,
        cost_estimate=pl.CostEstimate(flops=flops, transcendentals=0, bytes_accessed=14 << 20))(here, *arrays)
    return out if inverse is not None else out[0]


def device(tail, panel, rhs, block):
    k, _ = panel.shape
    cols = tail.shape[1]
    z, y = lax.axis_index("z"), lax.axis_index("y")
    x, core = lax.axis_index("x"), lax.axis_index("core")
    tail = tail.reshape(16, k, cols)
    i32 = lambda *v: jnp.stack([jnp.asarray(u, jnp.int32) for u in v])
    order = i32(y, (y + 3) % 4, (y + 1) % 4, (y + 2) % 4)
    here = i32(core, x)
    index = lambda dz: ((z + dz) % 4) * 4 + order
    ring = lambda i: i32(i, (i + 3) % 4, (i + 1) % 4, (i + 2) % 4)

    t0, = pick(tail, index(2)[:1], (1,))
    tf0 = shift(t0, "z", 2)
    wy = place([block, shift(block, "y", 1), shift(block, "y", -1), shift(block, "y", 2)], ring(y))
    top, bottom = panel[:TILE], panel[TILE:]
    l_t, r_b = shift(top, "y", 1), shift(bottom, "y", -1)
    l_b, r_t = shift(bottom, "y", 1), shift(top, "y", -1)
    wz = place([wy, shift(wy, "z", 1), shift(wy, "z", -1), shift(wy, "z", 2)], ring(z))
    tl, tr = pick(tail, jnp.concatenate([index(1), index(3)]), (4, 4))
    t1, t2, t_own = pick(tail, jnp.concatenate([index(2)[1:], index(0)]), (2, 1, 4))
    t_l = shift(tl, "z", 1)
    t_r = shift(tr, "z", -1)
    tf1 = shift(t1, "z", 2)
    tf2 = shift(t2, "z", 2)
    wx = [wz, shift(wz, "x", 1), shift(wz, "x", -1), shift(wz, "x", 2)]
    wx += [shift(w, "core", 1) for w in wx]
    f_l = shift(l_t, "y", 1)
    f_r = shift(r_b, "y", -1)
    inverse = invert(wx, jnp.concatenate([ring(x) * 2 + core, ring(x) * 2 + 1 - core]))

    near = [[panel], [l_t, l_b], [r_t, r_b]]
    far = [[f_l, f_r]]
    group = [t_own, t_l, t_r]
    c_0 = products(here, [[(tf0, 0)], [(t_own, 0)]], near[:1])
    c_g = products(
        here, [[None if t is t_own and j == 0 else (t, j) for j in range(3)] for t in group], near,
        start=(c_0, cols, cols), rhs=rhs)
    p_g = products(here, [[(t, 3)] for t in group], far, start=(c_g, 0, 3 * cols), inverse=inverse)
    c_f = products(here, [[(tf1, 0), (tf1, 1)]], near[1:], start=(c_0, 0, cols))
    p_f = products(here, [[(tf2, 0)]], far, start=(c_f, 0, cols), inverse=inverse)

    def over_rows(parts):
        mine, away = parts
        s = mine + shift(away, "core", 1)
        return (s[0] + shift(s[1], "x", 1)) + (shift(s[3], "x", -1) + shift(s[2], "x", 2))

    g = over_rows(p_g)
    h = over_rows(p_f)
    out = (g[0] + shift(g[1], "z", -1)) + (shift(g[2], "z", 1) + shift(h[0], "z", 2))
    return out.T


def solution(mesh):
    fine = Mesh(mesh.devices.reshape(4, 2, 4, 4), ("x", "core", "z", "y"))
    row, col = ("x", "core"), ("z", "y")
    in_specs = (P(row, col), P(row + col, None), P(row, col), P(row + col, None))
    return jax.shard_map(device, mesh=fine, in_specs=in_specs, out_specs=P(row, col), check_vma=False)
```
